32 devices in a mesh: cuts: 4 (over z), dp: 4 (over y, x), mp: 2 (over core).
Axes of the slice: x: 2, y: 2, z: 4, core: 2. Of those that a mesh axis runs over, the one named last changes fastest.
Arguments:
- attn_out: bfloat16 [2048, 3072], P(('cuts', 'dp'), 'mp'), may hold values from -6 to 6
- out_weight: bfloat16 [3072, 6144], P('mp'), may hold values from -0.109375 to 0.109375
- residual: bfloat16 [2048, 6144], P(('cuts', 'dp', 'mp')), may hold values from -45 to 45
- target: bfloat16 [2048, 6144], P(('cuts', 'dp', 'mp')), may hold values from -5 to 5
- norm_gain: float32 [6144], replicated, may hold values from 0.1 to 1.9
Outputs:
- block_out: bfloat16 [2048, 6144], P(('cuts', 'dp', 'mp'))
- attn_grad: bfloat16 [2048, 3072], P(('cuts', 'dp'), 'mp')
- weight_grad: float32 [3072, 6144], P('mp', 'dp')
The draws below stay inside these ranges and needn't reach their ends.
All inputs are finite; a program needn't handle non-finite values.
Results may differ from the reference program's by a relative error of at most 0.018.
Values may be sent and summed in bfloat16 or wider, within the bound.
No kernel may reach another device: no remote copies, remote signals or barrier semaphores. Data moves between devices by JAX's collectives and lax.ppermute only.
A program may use at most 128 MiB of HBM per device.

```python
import math
import jax
import jax.numpy as jnp
from jax import lax

D = 6144
TOK_DEV = 128
INNER = 3072
REPLICAS = 16
TOKENS = 2048
N_MP = 2


def draw_residual(key, part):
    key_rows = jax.random.fold_in(key, 11)
    key_cols = jax.random.fold_in(key, 12)
    key_base = jax.random.fold_in(key, 13)
    row_scale = jnp.exp(jax.random.uniform(key_rows, (TOKENS, 1), jnp.float32, math.log(0.3), math.log(3.0)))
    col_scale = jnp.exp(jax.random.uniform(key_cols, (1, D), jnp.float32, math.log(0.3), math.log(3.0)))
    base = jnp.clip(jax.random.normal(key_base, (TOKENS, D), jnp.float32), -5.0, 5.0)
    return (base * row_scale * col_scale).astype(jnp.bfloat16)


def draw_target(key, part):
    key_base = jax.random.fold_in(key, 21)
    key_offset = jax.random.fold_in(key, 22)
    offset = jax.random.uniform(key_offset, (TOKENS, 1), jnp.float32, -1.0, 1.0)
    base = jnp.clip(jax.random.normal(key_base, (TOKENS, D), jnp.float32), -4.0, 4.0)
    return (base + offset).astype(jnp.bfloat16)


def level_of(rng, extent, pieces, least, largest):
    level, own = 1.0, jax.random.fold_in(rng, 6)
    for position, shards_of in pieces:
        draws = jnp.exp(jax.random.uniform(jax.random.fold_in(own, position), (shards_of,), jnp.float32, least / len(pieces), largest / len(pieces)))
        level = level * jnp.repeat(draws, extent[position] // shards_of).reshape([-1 if axis == position else 1 for axis in range(len(extent))])
    return level


def scatter_about(stream_key, shape, width, limit, pieces=(), kind=jnp.bfloat16):
    gain = level_of(stream_key, shape, pieces, -0.22, 0.18) if pieces else 1.0
    array = jax.random.normal(stream_key, shape, jnp.float32) * width * gain
    return jnp.minimum(jnp.maximum(array, -limit), limit).astype(kind)


def setup_inputs(seed: int = 0) -> dict:
    seeds = jax.random.split(jax.random.key(seed), 6)
    return {
        "attn_out": scatter_about(seeds[0], (TOKENS, INNER), 1.0, 6.0, ((0, 16), (1, 2))),
        "out_weight": scatter_about(seeds[1], (INNER, D), INNER ** -0.5, 0.109375, ((0, 2),)),
        "residual": draw_residual(jax.random.fold_in(seeds[5], 71), 0),
        "target": draw_target(jax.random.fold_in(seeds[5], 71), 0),
        "norm_gain": jnp.clip(1.0 + 0.18 * jax.random.normal(seeds[4], (D,), jnp.float32), 0.1, 1.9),
    }


epsilon = 1e-06

def norm_backward(stream, target, norm_gain):
    center = stream - lax.optimization_barrier(jnp.mean(stream, axis=1, keepdims=True))
    inv_std = lax.rsqrt(lax.optimization_barrier(jnp.mean(center * center, axis=1, keepdims=True)) + epsilon)
    normed = center * inv_std
    misfit = normed * norm_gain[None, :] - target.astype(jnp.float32)
    gain_err = misfit * norm_gain[None, :]
    bracket = gain_err - lax.optimization_barrier(jnp.mean(gain_err, axis=1, keepdims=True)) - normed * lax.optimization_barrier(jnp.mean(gain_err * normed, axis=1, keepdims=True))
    return (inv_std * bracket).astype(jnp.bfloat16)

def reference(attn_out, out_weight, residual, target, norm_gain):
    group_cols = INNER // N_MP
    replica_scale = 1.0 / REPLICAS
    heads_all = attn_out.reshape(REPLICAS, TOK_DEV, INNER)
    resid_all = residual.reshape(REPLICAS, TOK_DEV, D)
    target_all = target.reshape(REPLICAS, TOK_DEV, D)

    def replica_step(grad_sum, inputs):
        head_block, resid_block, target_block = inputs
        stream = resid_block.astype(jnp.float32)
        for group_idx in range(N_MP):
            low = group_idx * group_cols
            partial_value = jnp.dot(head_block[:, low:low + group_cols], out_weight[low:low + group_cols], preferred_element_type=jnp.float32)
            stream = stream + lax.optimization_barrier(partial_value.astype(jnp.bfloat16)).astype(jnp.float32)
        cotangent = norm_backward(stream, target_block, norm_gain)
        attn_rows = lax.dot_general(cotangent, out_weight, (((1,), (1,)), ((), ())), preferred_element_type=jnp.float32).astype(jnp.bfloat16)
        shares = lax.dot_general(head_block, cotangent, (((0,), (0,)), ((), ())), preferred_element_type=jnp.float32) * replica_scale
        grad_sum = grad_sum + lax.optimization_barrier(shares.astype(jnp.bfloat16)).astype(jnp.float32)
        return (grad_sum, (stream.astype(jnp.bfloat16), attn_rows))
    grad_sum, outputs = lax.scan(replica_step, jnp.zeros((INNER, D), jnp.float32), (heads_all, resid_all, target_all))
    block_out, attn_grad = outputs
    return (block_out.reshape(TOKENS, D), attn_grad.reshape(TOKENS, INNER), grad_sum)
```

```python
import jax
import jax.numpy as jnp
from jax import lax
from jax.sharding import PartitionSpec as P

epsilon = 1e-06


f32 = jnp.float32
bf16 = jnp.bfloat16


def norm_backward(stream, target, norm_gain):
    center = stream - jnp.mean(stream, axis=1, keepdims=True)
    inv_std = lax.rsqrt(jnp.mean(center * center, axis=1, keepdims=True) + epsilon)
    normed = center * inv_std
    misfit = normed * norm_gain[None, :] - target.astype(f32)
    gain_err = misfit * norm_gain[None, :]
    bracket = (
        gain_err
        - jnp.mean(gain_err, axis=1, keepdims=True)
        - normed * jnp.mean(gain_err * normed, axis=1, keepdims=True)
    )
    return (inv_std * bracket).astype(bf16)


def shift(x, axis, by):
    size = lax.axis_size(axis)
    return lax.ppermute(x, axis, [(i, (i + by) % size) for i in range(size)])


def cross(x, axis, mask):
    size = lax.axis_size(axis)
    return lax.ppermute(x, axis, [(i, i ^ mask) for i in range(size)])


def line_plan(size):
    groups, held = [], {}
    count = [0] * size
    for hop in range(1, size):
        for z in range(size):
            for step in (1, -1) if z % 2 == 0 else (-1, 1):
                origin, source = z + step * hop, z + step
                if not 0 <= origin < size:
                    continue
                count[z] += 1
                fed = held[(source, origin)] if hop > 1 else None
                for number, (group_fed, slot, pairs) in enumerate(groups):
                    clash = any(a == source or b == z for a, b in pairs)
                    if group_fed == fed and slot == count[z] and not clash:
                        pairs.append((source, z))
                        held[(z, origin)] = number
                        break
                else:
                    held[(z, origin)] = len(groups)
                    groups.append((fed, count[z], [(source, z)]))
    return groups


def line_gather(x, axis):
    size = lax.axis_size(axis)
    parts, slots = [], [x] + [None] * (size - 1)
    for fed, slot, pairs in line_plan(size):
        part = lax.ppermute(x if fed is None else parts[fed], axis, pairs)
        parts.append(part)
        slots[slot] = part if slots[slot] is None else slots[slot] + part
    return slots


def plane_gather(x, axis):
    size = lax.axis_size(axis)
    if size != 4:
        return [x] + [cross(x, axis, mask) for mask in range(1, size)]
    half = x.shape[0] // 2
    near, far = cross(x, axis, 1), cross(x, axis, 2)
    upper = cross(near[:half], axis, 2)
    lower = cross(far[half:], axis, 1)
    return [x, near, far, jnp.concatenate([upper, lower])]


def gathered(attn_out, out_weight, residual, target, norm_gain):
    n_dp, n_mp = lax.axis_size("dp"), lax.axis_size("mp")
    me_dp, me_mp = lax.axis_index("dp"), lax.axis_index("mp")
    replica_scale = 1.0 / (lax.axis_size("cuts") * n_dp)
    tokens, heads = attn_out.shape
    rows = tokens // n_mp
    width = out_weight.shape[1]
    columns = width // n_dp

    turned = lax.dynamic_slice_in_dim(
        jnp.concatenate([attn_out, attn_out]), me_mp * rows, tokens, 0
    )
    attn_slots = line_gather(turned, "cuts")

    partial = jnp.dot(turned, out_weight, preferred_element_type=f32).astype(bf16)
    stream = residual.astype(f32) + partial[:rows].astype(f32)
    for j in range(1, n_mp):
        stream = stream + shift(partial[j * rows : (j + 1) * rows], "mp", j).astype(f32)
    block_out = stream.astype(bf16)
    cotangent = norm_backward(stream, target, norm_gain)

    cols = []
    for mask in range(n_dp):
        block = lax.dynamic_slice_in_dim(cotangent, (me_dp ^ mask) * columns, columns, 1)
        cols.append(block if mask == 0 else cross(block, "dp", mask))
    cols = jnp.concatenate(cols)

    whole = jnp.concatenate([cotangent] + [shift(cotangent, "mp", -j) for j in range(1, n_mp)])
    attn_grad = lax.dot_general(
        whole, out_weight, (((1,), (1,)), ((), ())), preferred_element_type=f32
    ).astype(bf16)
    attn_grad = lax.dynamic_slice_in_dim(
        jnp.concatenate([attn_grad, attn_grad]), tokens - me_mp * rows, tokens, 0
    )

    pieces = 2
    piece = columns // pieces
    cot_slots = [line_gather(cols[:, p * piece : (p + 1) * piece], "cuts") for p in range(pieces)]

    totals = [None] * pieces
    for slot in range(len(attn_slots)):
        blocks = plane_gather(attn_slots[slot], "dp")
        lhs = jnp.concatenate(
            [b[j * rows : (j + 1) * rows] for j in range(n_mp) for b in blocks]
        )
        for p in range(pieces):
            mine = cot_slots[p][slot]
            rhs = jnp.concatenate([mine] + [shift(mine, "mp", -j) for j in range(1, n_mp)])
            term = lax.dot_general(
                lhs, rhs, (((0,), (0,)), ((), ())), preferred_element_type=f32
            ) * replica_scale
            totals[p] = term if totals[p] is None else totals[p] + term
    return block_out, attn_grad, jnp.concatenate(totals, axis=1)


def summed(attn_out, out_weight, residual, target, norm_gain):
    tokens_dev, head_cols = attn_out.shape
    replica_scale = 1.0 / (lax.axis_size("cuts") * lax.axis_size("dp"))
    total = lax.psum_scatter(
        jnp.dot(attn_out, out_weight, preferred_element_type=f32).astype(bf16),
        "mp",
        scatter_dimension=0,
        tiled=True,
    ).astype(f32)
    stream = total + residual.astype(f32)
    block_out = stream.astype(bf16)
    cotangent = norm_backward(stream, target, norm_gain)
    portion = lax.all_gather(cotangent, "mp", axis=0, tiled=True)
    attn_grad = lax.dot_general(
        portion, out_weight, (((1,), (1,)), ((), ())), preferred_element_type=f32
    ).astype(bf16)
    columns = lax.all_to_all(portion, "dp", split_axis=1, concat_axis=0, tiled=True)
    heads = lax.all_gather(attn_out, "dp", axis=0, tiled=True)
    share = (
        lax.dot_general(heads, columns, (((0,), (0,)), ((), ())), preferred_element_type=f32)
        * replica_scale
    )
    weight_grad = lax.psum(share.astype(bf16), "cuts").astype(f32)
    return block_out, attn_grad, weight_grad


def per_device(attn_out, out_weight, residual, target, norm_gain):
    n_cuts, n_dp, n_mp = (lax.axis_size(a) for a in ("cuts", "dp", "mp"))
    tokens, heads = attn_out.shape
    columns = out_weight.shape[1] // n_dp
    row_values = (n_cuts - 1) * tokens * (heads + n_dp * columns // n_mp)
    use_rows = row_values <= heads * columns and n_dp & (n_dp - 1) == 0
    form = gathered if use_rows else summed
    return form(attn_out, out_weight, residual, target, norm_gain)


def solution(mesh):
    placed = (
        P(("cuts", "dp"), "mp"),
        P("mp", None),
        P(("cuts", "dp", "mp"), None),
        P(("cuts", "dp", "mp"), None),
        P(),
    )
    return jax.shard_map(
        per_device,
        mesh=mesh,
        in_specs=placed,
        out_specs=(P(("cuts", "dp", "mp"), None), P(("cuts", "dp"), "mp"), P("mp", "dp")),
        check_vma=False,
    )
```

```python
import functools

import jax
import jax.numpy as jnp
from jax import lax
from jax.experimental import pallas as pl
from jax.experimental.pallas import tpu as pltpu
from jax.sharding import PartitionSpec as P


epsilon = 1e-06


f32 = jnp.float32
bf16 = jnp.bfloat16


def norm_backward(stream, target, norm_gain):
    center = stream - jnp.mean(stream, axis=1, keepdims=True)
    inv_std = lax.rsqrt(jnp.mean(center * center, axis=1, keepdims=True) + epsilon)
    normed = center * inv_std
    misfit = normed * norm_gain[None, :] - target.astype(f32)
    gain_err = misfit * norm_gain[None, :]
    bracket = (
        gain_err
        - jnp.mean(gain_err, axis=1, keepdims=True)
        - normed * jnp.mean(gain_err * normed, axis=1, keepdims=True)
    )
    return (inv_std * bracket).astype(bf16)


ROW, PLANE, PAIR = 4, 4, 2


def swap_cores(x):
    return lax.ppermute(x, "mp", [(0, 1), (1, 0)])


def row_first(x):
    far = lax.ppermute(x, "cuts", [(i, i ^ 2) for i in range(ROW)])
    near = lax.ppermute(x, "cuts", [(i, i ^ 1) for i in range(ROW)])
    return near, far


def row_last(x, far):
    ends = lax.ppermute(far, "cuts", [(1, 0), (2, 3)])
    middle = lax.ppermute(x, "cuts", [(1, 2), (2, 1)])
    return ends, middle


def after(event, xs):
    return list(lax.optimization_barrier((*xs, event))[:-1])


def per_core(pairs_0, pairs_1):
    return [(a * PAIR + m, b * PAIR + m) for m, p in enumerate((pairs_0, pairs_1)) for a, b in p]


FIRST = per_core([(i, i ^ 2) for i in range(ROW)], [(i, i ^ 1) for i in range(ROW)])
ENDS = per_core([(1, 0), (2, 3)], [])
MIDDLE = per_core([], [(1, 2), (2, 1)])


def plane_step(x, turn):
    pairs = []
    for d in range(PLANE):
        for m in range(PAIR):
            other = d ^ (1 if m == turn else 2)
            pairs.append((d * PAIR + m, other * PAIR + m))
    return lax.ppermute(x, ("dp", "mp"), pairs)


def plane_gather(x):
    first = plane_step(x, 0)
    second = plane_step(x, 1)
    return [x, first, second, plane_step(first, 1)]


OTHER = (0, 2, 1, 3)

VMEM_FIRST, VMEM_LAST, VMEM_BACK = 26 << 20, 26 << 20, 46 << 20


def grad_kernel(counts, has_total, scale, info_ref, *refs):
    ins, (out_ref, rhs_ref) = list(refs[:-2]), refs[-2:]
    total_ref = ins.pop(0) if has_total else None
    terms = []
    for count in counts:
        terms.append((ins[:4], ins[4 : 4 + count]))
        ins = ins[4 + count :]
    rows = terms[0][1][0].shape[0] // (PLANE * PAIR)

    @pl.when(pl.program_id(0) == 0)
    def _():
        core = info_ref[0]
        for t, (_, rights) in enumerate(terms):
            view = info_ref[1 + t]
            for half in range(PAIR):
                owner = view if half == 0 else 1 - view
                for j in range(PLANE):
                    block = half * PLANE + jnp.where(owner == core, j, OTHER[j])
                    source = pl.ds(pl.multiple_of(block * rows, rows), rows)
                    block = j * PAIR + owner
                    target = pl.ds(pl.multiple_of(block * rows, rows), rows)
                    value = rights[0][source, :]
                    for r in rights[1:]:
                        value = value + r[source, :]
                    rhs_ref[t, target, :] = value

    acc = None
    for t, (lefts, _) in enumerate(terms):
        lhs = jnp.concatenate([r[0] for r in lefts], axis=1)
        part = jnp.dot(lhs, rhs_ref[t], preferred_element_type=f32)
        acc = part if acc is None else acc + part
    acc = acc * scale
    if total_ref is not None:
        acc = acc + total_ref[...].astype(f32)
    out_ref[...] = acc.astype(out_ref.dtype)


def add_terms(total, out, shape, dtype, terms, info, start, scale, limit):
    heads = shape[0]
    depth, width = terms[0][1][0].shape
    tile = heads // 2
    args, specs, aliases = [], [], {}
    if out is not None:
        args.append(out)
        specs.append(pl.BlockSpec(memory_space=pl.ANY))
        aliases = {1: 0}
    if total is not None:
        args.append(total)
        specs.append(pl.BlockSpec((tile, width), lambda i, c: (i, 0)))
    n_terms = len(terms)
    for t, (blocks, rights) in enumerate(terms):
        at = 1 + n_terms + t
        for b in blocks:
            args.append(b)
            specs.append(pl.BlockSpec((1, tile, b.shape[2]), lambda i, c, at=at: (c[at], i, 0)))
        for r in rights:
            args.append(r)
            specs.append(pl.BlockSpec(r.shape, lambda i, c: (0, 0)))
    counts = tuple(len(rights) for _, rights in terms)
    kernel = functools.partial(grad_kernel, counts, total is not None, scale)
    if out is not None:
        inner = kernel

        def kernel(info_ref, _, *refs):
            inner(info_ref, *refs)

    return pl.pallas_call(
        kernel,
        grid_spec=pltpu.PrefetchScalarGridSpec(
            num_scalar_prefetch=1,
            grid=(heads // tile,),
            in_specs=specs,
            out_specs=pl.BlockSpec((tile, width), lambda i, c: (i, start // width)),
            scratch_shapes=[pltpu.VMEM((n_terms, depth, width), bf16)],
        ),
        out_shape=jax.ShapeDtypeStruct(shape, dtype),
        input_output_aliases=aliases,
        cost_estimate=pl.CostEstimate(
            flops=2 * heads * width * depth * n_terms,
            bytes_accessed=8 * heads * width,
            transcendentals=0,
        ),
        compiler_params=pltpu.CompilerParams(vmem_limit_bytes=limit),
        name="weight_grad_step",
    )(info, *args)


def back_kernel(core_ref, mine_ref, theirs_ref, weight_ref, *refs):
    out_ref, rows_ref = refs[-2:]
    rows = mine_ref.shape[0]

    @pl.when(pl.program_id(0) == 0)
    def _():
        core = core_ref[0]
        rows_ref[pl.ds(pl.multiple_of(core * rows, rows), rows), :] = mine_ref[...]
        rows_ref[pl.ds(pl.multiple_of((1 - core) * rows, rows), rows), :] = theirs_ref[...]

    out_ref[...] = lax.dot_general(
        rows_ref[...], weight_ref[...], (((1,), (1,)), ((), ())), preferred_element_type=f32
    ).astype(bf16)


def back_rows(part, parts, out, mine, theirs, weight, core):
    rows, width = mine.shape
    heads = weight.shape[0]
    tile = 256
    steps = heads // tile // parts
    specs = [
        pl.BlockSpec((rows, width), lambda i, c: (0, 0)),
        pl.BlockSpec((rows, width), lambda i, c: (0, 0)),
        pl.BlockSpec((tile, width), lambda i, c: (part * steps + i, 0)),
    ]
    args = [mine, theirs, weight]
    if out is not None:
        specs.append(pl.BlockSpec(memory_space=pl.ANY))
        args.append(out)
    return pl.pallas_call(
        back_kernel,
        grid_spec=pltpu.PrefetchScalarGridSpec(
            num_scalar_prefetch=1,
            grid=(steps,),
            in_specs=specs,
            out_specs=pl.BlockSpec((PAIR * rows, tile), lambda i, c: (0, part * steps + i)),
            scratch_shapes=[pltpu.VMEM((PAIR * rows, width), bf16)],
        ),
        out_shape=jax.ShapeDtypeStruct((PAIR * rows, heads), bf16),
        input_output_aliases={} if out is None else {4: 0},
        cost_estimate=pl.CostEstimate(
            flops=2 * PAIR * rows * width * heads // parts,
            bytes_accessed=2 * width * heads // parts,
            transcendentals=0,
        ),
        compiler_params=pltpu.CompilerParams(vmem_limit_bytes=VMEM_BACK),
        name="attn_grad",
    )(core, *args)


def gathered(attn_out, out_weight, residual, target, norm_gain):
    me_dp, me_mp = lax.axis_index("dp"), lax.axis_index("mp")
    core = me_mp.astype(jnp.int32).reshape(1)
    replica_scale = 1.0 / (ROW * PLANE)
    tokens, heads = attn_out.shape
    rows = tokens // PAIR
    width = out_weight.shape[1]
    columns = width // PLANE
    shape = (heads, columns)

    lifted = lax.optimization_barrier(attn_out.T)[None]
    a_near, a_far = row_first(lifted)
    own_blocks = plane_gather(lifted)

    partial = jnp.dot(attn_out, out_weight, preferred_element_type=f32).astype(bf16)
    other = lax.dynamic_slice_in_dim(partial, (1 - me_mp) * rows, rows, 0)
    own = lax.dynamic_slice_in_dim(partial, me_mp * rows, rows, 0)
    stream = residual.astype(f32) + own.astype(f32) + swap_cores(other).astype(f32)
    block_out = stream.astype(bf16)
    cotangent = norm_backward(stream, target, norm_gain)

    masks = (0, 1 + me_mp, 2 - me_mp, 3)
    blocks = [
        lax.dynamic_slice_in_dim(cotangent, (me_dp ^ m) * columns, columns, 1) for m in masks
    ]
    cols = jnp.concatenate(
        [
            blocks[0],
            plane_step(blocks[1], 0),
            plane_step(blocks[2], 1),
            lax.ppermute(blocks[3], "dp", [(d, d ^ 3) for d in range(PLANE)]),
        ]
    )
    theirs = swap_cores(cotangent)
    attn_grad = None
    for part in range(1):
        attn_grad = back_rows(part, 1, attn_grad, cotangent, theirs, out_weight, core)

    a_ends, a_mid = row_last(lifted, a_far)
    a_near, a_far = after(theirs, (a_near, a_far))
    more = jnp.concatenate([a_near, a_far])
    first_blocks = plane_gather(more)
    a_last = jnp.add(*after(attn_grad, (a_ends, a_mid)))
    last_blocks = plane_gather(a_last)

    cols = jnp.concatenate([cols, swap_cores(cols)])
    ends_at = (columns - columns // 3, columns)
    pieces = len(ends_at)
    row = ("cuts", "mp")
    own, first, last = [], [], []
    parts = [cols[:, i:j] for i, j in zip((0, *ends_at), ends_at)]
    for x in lax.optimization_barrier(parts):
        y = lax.ppermute(x, row, FIRST)
        ends, middle = lax.ppermute(y, row, ENDS), lax.ppermute(x, row, MIDDLE)
        own.append((own_blocks, (x,)))
        first.append([(first_blocks, (y,)), (first_blocks, (swap_cores(y),))])
        sides = (ends, swap_cores(ends), middle, swap_cores(middle))
        last.append((last_blocks, sides))

    me_row = lax.axis_index("cuts")
    inner = jnp.where((me_row == 0) | (me_row == ROW - 1), 0, 1)

    def info(*entries):
        table = jnp.array(entries, jnp.int32)
        return table[:, 0] + table[:, 1] * me_mp + table[:, 2] * inner

    here, there, fixed = (0, 1, 0), (1, -1, 0), (0, 0, 0)
    info_first = info(here, here, here, there, fixed, there, here)
    info_last = info(here, (0, 0, 1), fixed)

    totals = []
    for p in range(pieces):
        terms = [own[p], *first[p]]
        part = (heads, parts[p].shape[1])
        limit = VMEM_LAST if p == 0 else VMEM_FIRST
        totals.append(add_terms(None, None, part, bf16, terms, info_first, 0, replica_scale, limit))
    grad = None
    for p in range(pieces):
        terms = [last[p]]
        grad = add_terms(
            totals[p],
            grad,
            shape,
            f32,
            terms,
            info_last,
            (0, *ends_at)[p],
            replica_scale,
            VMEM_LAST,
        )
    return block_out, attn_grad, grad


def summed(attn_out, out_weight, residual, target, norm_gain):
    replica_scale = 1.0 / (lax.axis_size("cuts") * lax.axis_size("dp"))
    total = lax.psum_scatter(
        jnp.dot(attn_out, out_weight, preferred_element_type=f32).astype(bf16),
        "mp",
        scatter_dimension=0,
        tiled=True,
    ).astype(f32)
    stream = total + residual.astype(f32)
    block_out = stream.astype(bf16)
    cotangent = norm_backward(stream, target, norm_gain)
    portion = lax.all_gather(cotangent, "mp", axis=0, tiled=True)
    attn_grad = lax.dot_general(
        portion, out_weight, (((1,), (1,)), ((), ())), preferred_element_type=f32
    ).astype(bf16)
    columns = lax.all_to_all(portion, "dp", split_axis=1, concat_axis=0, tiled=True)
    heads = lax.all_gather(attn_out, "dp", axis=0, tiled=True)
    share = (
        lax.dot_general(heads, columns, (((0,), (0,)), ((), ())), preferred_element_type=f32)
        * replica_scale
    )
    weight_grad = lax.psum(share.astype(bf16), "cuts").astype(f32)
    return block_out, attn_grad, weight_grad


def rows_form(sizes, tokens, heads, width):
    columns = width // sizes[1]
    row_values = (sizes[0] - 1) * tokens * (heads + sizes[1] * columns // sizes[2])
    return sizes == (ROW, PLANE, PAIR) and row_values <= heads * columns


def per_device(attn_out, out_weight, residual, target, norm_gain):
    sizes = tuple(lax.axis_size(a) for a in ("cuts", "dp", "mp"))
    form = gathered if rows_form(sizes, *attn_out.shape, out_weight.shape[1]) else summed
    return form(attn_out, out_weight, residual, target, norm_gain)


def solution(mesh):
    placed = (
        P(("cuts", "dp"), "mp"),
        P("mp", None),
        P(("cuts", "dp", "mp"), None),
        P(("cuts", "dp", "mp"), None),
        P(),
    )
    return jax.shard_map(
        per_device,
        mesh=mesh,
        in_specs=placed,
        out_specs=(P(("cuts", "dp", "mp"), None), P(("cuts", "dp"), "mp"), P("mp", "dp")),
        check_vma=False,
    )
```
